32 devices in a mesh: dp: 4 (over y, x), seq: 8 (over z, core).
Axes of the slice: x: 2, y: 2, z: 4, core: 2. Of those that a mesh axis runs over, the one named last changes fastest.
Arguments:
- stream: bfloat16 [4, 256, 1536], P('dp', 'seq'), may hold values from -6 to 6
- queries: bfloat16 [4, 256, 1536], P('dp', 'seq'), may hold values from -30 to 30
- new_keys: bfloat16 [4, 256, 1536], P('dp', 'seq'), may hold values from -6.5 to 6.5
- new_values: bfloat16 [4, 256, 1536], P('dp', 'seq'), may hold values from -6 to 6
- cache_keys: bfloat16 [4, 768, 1536], P('dp', 'seq'), may hold values from -6.375 to 6.375
- cache_values: bfloat16 [4, 768, 1536], P('dp', 'seq'), may hold values from -6 to 6
- cache_frames: int32 [4, 768], P('dp', 'seq'), may hold values from 0 to 20, as said below
- group_index: int32 [4], P('dp'), may hold values from 4 to 7, as said below
- timestep: int32 [4], P('dp'), may hold values from 0 to 3
- gate_table: float32 [4, 1536], replicated, may hold values from 0.1 to 1.9
- attn_out_weight: bfloat16 [1536, 1536], replicated, may hold values from -0.15625 to 0.15625
- critic_in: bfloat16 [32768, 1536], P(('dp', 'seq')), may hold values from -6 to 6
- critic_cot: bfloat16 [32768, 1536], P(('dp', 'seq')), may hold values from -6 to 6
- critic_weight: bfloat16 [1536, 1536], P(('dp', 'seq')), may hold values from -0.15625 to 0.15625
Outputs:
- stream_out: bfloat16 [4, 256, 1536], P('dp', 'seq')
- critic_grad_in: bfloat16 [32768, 1536], P(('dp', 'seq'))
- critic_grad_weight: float32 [1536, 1536], P(('dp', 'seq'))
The draws below stay inside these ranges and needn't reach their ends.
Inputs may be any that keep to these rules, and one draw needn't show every extreme that they name: `group_index`: index of the frame group; both ends are reached in every draw. `cache_frames`: sample b's cache holds the 12 frames 3 * group_index[b] - 12 to 3 * group_index[b] - 1, each in one contiguous run of slots, runs of equal length up to one slot, in a rotated order.
All inputs are finite; a program needn't handle non-finite values.
Results may differ from the reference program's by a relative error of at most 0.0045.
Values may be sent and summed in bfloat16 or wider, within the bound.
A program may use at most 128 MiB of HBM per device.

```python
import jax
import jax.numpy as jnp
from jax import lax

D = 1536
HEADS = 12
HEAD = 128
STEPS = 4
FRAMES_GROUP = 3
WINDOW_FRAMES = 9
BATCH = 4
GROUP = 256
CACHE = 768
CRIT_ROWS = 32768


def drawn_pair(key):
    base = jax.random.fold_in(key, 4711)
    key_q, key_k = jax.random.split(base, 2)
    query_draw = jnp.clip(1.6 * jax.random.normal(key_q, (BATCH, GROUP, D), jnp.float32), -6.4, 6.4)
    key_draw = jnp.clip(1.6 * jax.random.normal(key_k, (BATCH, GROUP, D), jnp.float32), -6.4, 6.4)
    return (query_draw, key_draw)


def draw_queries(key, part):
    return drawn_pair(key)[0].astype(jnp.bfloat16)


def draw_new_keys(key, part):
    return drawn_pair(key)[1].astype(jnp.bfloat16)


def frame_layout(key):
    base = jax.random.fold_in(key, 9173)
    key_group, key_turn = jax.random.split(base, 2)
    cycle = FRAMES_GROUP + WINDOW_FRAMES
    group = jax.random.randint(key_group, (BATCH,), 4, 8, dtype=jnp.int32)
    group = group.at[0].set(7).at[BATCH - 1].set(4)
    turn = jax.random.randint(key_turn, (BATCH, 1), 0, cycle, dtype=jnp.int32)
    block = jnp.arange(CACHE, dtype=jnp.int32) * cycle // CACHE
    frames = FRAMES_GROUP * group[:, None] - cycle + (block[None, :] + turn) % cycle
    return (group, frames.astype(jnp.int32))


def draw_group_index(key, part):
    return frame_layout(key)[0]


def draw_cache_frames(key, part):
    return frame_layout(key)[1]


def plant(drawn, own_key, low, top_value):
    longest = drawn.shape.index(max(drawn.shape))
    spots = []
    for shift in (0, 1):
        where = [jax.random.randint(jax.random.fold_in(own_key, axis), (), 0, length) for axis, length in enumerate(drawn.shape)]
        where[longest] = (where[longest] + shift) % drawn.shape[longest]
        spots.append(tuple(where))
    return drawn.at[spots[0]].set(low).at[spots[1]].set(top_value)


def strengthened(entries, stream_key, source, target, parts, factor):
    def block_of(axis_at):
        return (jnp.arange(entries.shape[axis_at]) // (entries.shape[axis_at] // parts)).reshape((-1,) + (1,) * (entries.ndim - 1 - axis_at))

    one_side = jax.random.permutation(stream_key, parts)[block_of(target)]
    other_side = (block_of(target) + parts // 2) % parts
    return jnp.where((block_of(source) == one_side) | (block_of(source) == other_side), factor * entries, entries)


def shard_levels(key, shape, cuts, least, largest):
    def one(position, shards_of):
        heights = jax.random.uniform(jax.random.fold_in(jax.random.fold_in(key, 6), position), (shards_of,), jnp.float32, least / len(cuts), largest / len(cuts))
        return jnp.repeat(jnp.exp(heights), shape[position] // shards_of).reshape((-1,) + (1,) * (len(shape) - position - 1))

    loudness = one(*cuts[0])
    for cut in cuts[1:]:
        loudness = loudness * one(*cut)
    return loudness


def noise(key, shape, spread, limit, cuts=(), held_as=jnp.bfloat16):
    factor_of = shard_levels(key, shape, cuts, -0.22, 0.18) if cuts else 1.0
    values = jax.random.normal(key, shape, jnp.float32) * spread * factor_of
    return jnp.minimum(jnp.maximum(values, -limit), limit).astype(held_as)


def noise_with(key, shape, scale, bound, cuts, heavy, kind=jnp.bfloat16):
    array = scale * jax.random.normal(key, shape, jnp.float32)
    if cuts:
        array = array * shard_levels(key, shape, cuts, -0.22, 0.18)
    return jnp.clip(strengthened(array, jax.random.fold_in(key, 3), *heavy), -bound, bound).astype(kind)


def setup_inputs(seed: int = 0) -> dict:
    key_list = jax.random.split(jax.random.key(seed), 15)
    stream = noise(key_list[0], (BATCH, GROUP, D), 1.0, 6.0, ((0, 4), (1, 8)))
    queries = draw_queries(jax.random.fold_in(key_list[14], 71), 0)
    new_keys = draw_new_keys(jax.random.fold_in(key_list[14], 71), 0)
    new_values = noise(key_list[3], (BATCH, GROUP, D), 1.0, 6.0, ((0, 4), (1, 8)))
    cache_keys = noise(key_list[4], (BATCH, CACHE, D), 1.6, 6.375, ((0, 4), (1, 8)))
    cache_values = noise(key_list[5], (BATCH, CACHE, D), 1.0, 6.0, ((0, 4), (1, 8)))
    cache_frames = draw_cache_frames(jax.random.fold_in(key_list[14], 71), 0)
    group_index = draw_group_index(jax.random.fold_in(key_list[14], 71), 0)
    timestep = plant(jax.random.randint(key_list[8], (BATCH,), 0, STEPS), jax.random.fold_in(key_list[8], 1), 0, STEPS - 1).astype(jnp.int32)
    gate_table = jnp.clip(1.0 + 0.18 * jax.random.normal(key_list[9], (STEPS, D), jnp.float32), 0.1, 1.9)
    attn_out_weight = noise(key_list[10], (D, D), D ** -0.5, 0.15625)
    critic_in = noise_with(key_list[11], (CRIT_ROWS, D), 1.0, 6.0, ((0, 32),), (0, 1, 32, 2.75))
    critic_cot = noise(key_list[12], (CRIT_ROWS, D), 1.0, 6.0, ((0, 32),))
    critic_weight = noise(key_list[13], (D, D), D ** -0.5, 0.15625, ((0, 32),))
    return {"stream": stream, "queries": queries, "new_keys": new_keys, "new_values": new_values, "cache_keys": cache_keys, "cache_values": cache_values, "cache_frames": cache_frames, "group_index": group_index, "timestep": timestep, "gate_table": gate_table, "attn_out_weight": attn_out_weight, "critic_in": critic_in, "critic_cot": critic_cot, "critic_weight": critic_weight}


def attend_sample(packed):
    query_block, key_new, value_new, key_cache, value_cache, frames, group = packed
    keys = jnp.concatenate([key_cache, key_new], axis=0)
    values = jnp.concatenate([value_cache, value_new], axis=0)
    first = FRAMES_GROUP * group
    live_cache = (frames < first) & (frames >= first - WINDOW_FRAMES)
    live = jnp.concatenate([live_cache, jnp.ones((GROUP,), dtype=bool)])
    query_heads = query_block.reshape(GROUP, HEADS, HEAD).transpose(1, 0, 2)
    key_heads = keys.reshape(GROUP + CACHE, HEADS, HEAD).transpose(1, 0, 2)
    value_heads = values.reshape(GROUP + CACHE, HEADS, HEAD).transpose(1, 0, 2)

    def one_head(triple):
        q_head, k_head, v_head = triple
        scores = jnp.dot(q_head, k_head.T, preferred_element_type=jnp.float32) * (HEAD ** -0.5)
        scores = jnp.where(live[None, :], scores, -1e30)
        top = jnp.max(scores, axis=1, keepdims=True)
        weights = jnp.where(live[None, :], jnp.exp(scores - top), 0.0)
        totals = jnp.sum(weights, axis=1, keepdims=True)
        summed = jnp.dot(weights.astype(jnp.bfloat16), v_head, preferred_element_type=jnp.float32)
        return summed / totals

    mixed = lax.map(one_head, (query_heads, key_heads, value_heads))
    return mixed.transpose(1, 0, 2).reshape(GROUP, D).astype(jnp.bfloat16)


def reference(stream, queries, new_keys, new_values, cache_keys, cache_values, cache_frames, group_index, timestep, gate_table, attn_out_weight, critic_in, critic_cot, critic_weight):
    mixed = lax.map(attend_sample, (queries, new_keys, new_values, cache_keys, cache_values, cache_frames, group_index))
    projected = jnp.dot(mixed.reshape(BATCH * GROUP, D), attn_out_weight, preferred_element_type=jnp.float32).reshape(BATCH, GROUP, D)
    onehot = (timestep[:, None] == jnp.arange(STEPS, dtype=jnp.int32)[None, :]).astype(jnp.float32)
    gate = jnp.dot(onehot, gate_table, precision=lax.Precision.HIGHEST)
    stream_out = (stream.astype(jnp.float32) + gate[:, None, :] * projected).astype(jnp.bfloat16)
    grad_in = jnp.dot(critic_cot, critic_weight.T, preferred_element_type=jnp.float32).astype(jnp.bfloat16)
    grad_weight = jnp.dot(critic_in.T, critic_cot, preferred_element_type=jnp.float32) * (float(CRIT_ROWS) ** -0.5)
    return (stream_out, grad_in, grad_weight)
```

```python
import functools

import jax
import jax.numpy as jnp
from jax import lax
from jax.experimental import pallas as pl
from jax.experimental.pallas import tpu as pltpu
from jax.sharding import PartitionSpec as P

HEADS = 12
HEAD = 128
FRAMES_GROUP = 3
WINDOW_FRAMES = 9


def critic_pass(critic_in, critic_cot, critic_weight):
    grad_in = lax.dot_general(
        critic_cot,
        lax.all_gather(critic_weight, ("dp", "seq"), axis=0, tiled=True),
        (((1,), (1,)), ((), ())),
        preferred_element_type=jnp.float32,
    ).astype(jnp.bfloat16)
    factor = float(critic_in.shape[0] * lax.axis_size(("dp", "seq"))) ** (-0.5)
    whole_term = (
        lax.dot_general(
            critic_in, critic_cot, (((0,), (0,)), ((), ())), preferred_element_type=jnp.float32
        )
        * factor
    )
    grad_weight = lax.psum_scatter(whole_term, ("dp", "seq"), scatter_dimension=0, tiled=True)
    return (grad_in, grad_weight)


def by_collectives(
    stream,
    queries,
    new_keys,
    new_values,
    cache_keys,
    cache_values,
    cache_frames,
    group_index,
    timestep,
    gate_table,
    attn_out_weight,
    critic_in,
    critic_cot,
    critic_weight,
):
    query_local = queries[0]
    own_rows = query_local.shape[0]
    width = query_local.shape[1]
    scale = HEAD ** (-0.5)
    first_frame = FRAMES_GROUP * group_index[0]
    frames = cache_frames[0]
    live_cache = (frames < first_frame) & (frames >= first_frame - WINDOW_FRAMES)
    live_local = jnp.concatenate([live_cache, jnp.ones((own_rows,), dtype=bool)])
    keys_local = jnp.concatenate([cache_keys[0], new_keys[0]], axis=0)
    values_local = jnp.concatenate([cache_values[0], new_values[0]], axis=0)
    all_queries = lax.all_gather(queries, "seq", axis=1, tiled=True)[0]
    total_rows = all_queries.shape[0]
    query_heads = all_queries.reshape(total_rows, HEADS, HEAD)
    key_heads = keys_local.reshape(-1, HEADS, HEAD)
    value_heads = values_local.reshape(-1, HEADS, HEAD)
    scores = (
        jnp.einsum("qhd,khd->hqk", query_heads, key_heads, preferred_element_type=jnp.float32)
        * scale
    )
    scores = jnp.where(live_local[None, None, :], scores, -1e30)
    local_top = jnp.max(scores, axis=2)
    global_top = lax.pmax(local_top, "seq")
    weights = jnp.where(live_local[None, None, :], jnp.exp(scores - global_top[:, :, None]), 0.0)
    totals = jnp.sum(weights, axis=2)
    summed = jnp.einsum(
        "hqk,khd->qhd",
        weights.astype(jnp.bfloat16),
        value_heads,
        preferred_element_type=jnp.float32,
    )
    own_sums, own_totals = (
        lax.psum_scatter(summed.reshape(total_rows, width), "seq", scatter_dimension=0, tiled=True),
        lax.psum_scatter(totals.T, "seq", scatter_dimension=0, tiled=True),
    )
    mixed = (
        (own_sums.reshape(own_rows, HEADS, HEAD) / own_totals[:, :, None])
        .reshape(own_rows, width)
        .astype(jnp.bfloat16)
    )
    projected = jnp.dot(mixed, attn_out_weight, preferred_element_type=jnp.float32)
    onehot = (
        timestep[:, None] == jnp.arange(gate_table.shape[0], dtype=jnp.int32)[None, :]
    ).astype(jnp.float32)
    gate = jnp.dot(onehot, gate_table, precision=lax.Precision.HIGHEST)
    stream_out = (stream[0].astype(jnp.float32) + gate * projected).astype(jnp.bfloat16)[None]
    grad_in, grad_weight = critic_pass(critic_in, critic_cot, critic_weight)
    return (stream_out, grad_in, grad_weight)


def step_kernel(
    zs,
    parts,
    stream,
    queries,
    new_keys,
    new_values,
    cache_keys,
    cache_values,
    frames,
    group_index,
    timestep,
    gate_table,
    out_weight_hbm,
    critic_in_hbm,
    critic_cot_hbm,
    weight_shard,
    stream_out,
    grad_in_hbm,
    grad_weight,
    cin,
    cot,
    out_weight,
    wfull,
    gmine,
    psend,
    precv,
    dsend,
    xsend,
    ysend,
    rx_diag,
    ry_diag,
    rx_block,
    ry_block,
    osum,
    zsend,
    zrecv,
    gin,
    q_all,
    kfull,
    vfull,
    frames_recv,
    live_row,
    asend,
    arecv,
    ssend,
    srecv,
    mixed,
    send_sems,
    recv_sems,
    local_sems,
):
    f32, bf16 = jnp.float32, jnp.bfloat16
    dp, seq = lax.axis_index("dp"), lax.axis_index("seq")
    z, core = seq // 2, lax.rem(seq, 2)
    other = 1 - core
    tokens, width = cin.shape
    block = width // 4
    shard = block // (2 * zs)
    half = width // 2
    own_q = queries.shape[0]
    cached, fresh = cache_keys.shape[0], new_keys.shape[0]
    keys_one = cached + fresh
    heads_here = half // HEAD
    zh = zs // 2
    dp_x = dp + 1 - 2 * lax.rem(dp, 2)
    dp_y = lax.rem(dp + 2, 4)
    dp_d = dp_x + 2 - 4 * (dp_x // 2)
    order = (dp_d, dp_x, dp_y, dp)
    xn, yn, pair = (dp_x, seq), (dp_y, seq), (dp, z * 2 + other)

    loads = [
        pltpu.make_async_copy(critic_in_hbm, cin, local_sems.at[0]),
        pltpu.make_async_copy(critic_cot_hbm, cot, local_sems.at[1]),
        pltpu.make_async_copy(out_weight_hbm, out_weight, local_sems.at[2]),
    ]
    for load in loads:
        load.start()

    group = []
    for j in range(zs):
        for cc in range(2):
            if j or cc:
                zt = lax.rem(z + j, zs)
                ct = core if cc == 0 else other
                group.append((j, cc, zt, ct))
    barrier = pltpu.get_barrier_semaphore()
    peers = [xn, yn] + [(dp, zt * 2 + ct) for (_, _, zt, ct) in group]
    for peer in peers:
        pl.semaphore_signal(
            barrier, inc=1, device_id=peer, device_id_type=pl.DeviceIdType.MESH
        )
    pl.semaphore_wait(barrier, len(peers))

    sent = []

    def send(src, dst, peer):
        n = len(sent)
        copy = pltpu.make_async_remote_copy(
            src_ref=src,
            dst_ref=dst,
            send_sem=send_sems.at[n],
            recv_sem=recv_sems.at[n],
            device_id=peer,
            device_id_type=pl.DeviceIdType.MESH,
        )
        copy.start()
        sent.append(copy)
        return copy

    other_cols = pl.ds(pl.multiple_of(other * half, 128), half)
    own_cols = pl.ds(pl.multiple_of(core * half, 128), half)

    early = []
    for j, cc, zt, ct in group:
        cols = own_cols if cc == 0 else other_cols
        early.append(send(queries.at[:, cols], q_all.at[seq], (dp, zt * 2 + ct)))
    early.append(
        send(cache_keys.at[:, other_cols], kfull.at[pl.ds(keys_one, cached)], pair)
    )
    early.append(
        send(new_keys.at[:, other_cols], kfull.at[pl.ds(keys_one + cached, fresh)], pair)
    )
    early.append(
        send(cache_values.at[:, other_cols], vfull.at[pl.ds(keys_one, cached)], pair)
    )
    early.append(
        send(new_values.at[:, other_cols], vfull.at[pl.ds(keys_one + cached, fresh)], pair)
    )
    early.append(send(frames, frames_recv, pair))
    w_z = []
    for j in range(1, zs):
        zt = lax.rem(z + j, zs)
        w_z.append(send(weight_shard, wfull.at[dp, z, core], (dp, zt * 2 + core)))

    wfull[dp, z, core] = weight_shard[...]
    q_all[seq] = queries[:, own_cols]
    kfull[0:cached] = cache_keys[:, own_cols]
    kfull[cached:keys_one] = new_keys[:, own_cols]
    vfull[0:cached] = cache_values[:, own_cols]
    vfull[cached:keys_one] = new_values[:, own_cols]

    loads[0].wait()
    loads[1].wait()
    tile = 512 if width % 512 == 0 else 128

    def grad_block(b):
        rows = pl.ds(pl.multiple_of(order[b] * block, 128), block)

        def body(t, carry):
            cols = pl.ds(pl.multiple_of(t * tile, tile), tile)
            acc = lax.dot_general(
                cin[:, rows],
                cot[:, cols],
                (((0,), (0,)), ((), ())),
                preferred_element_type=f32,
            )
            for k in range(zs):
                lo = acc[2 * k * shard : (2 * k + 1) * shard]
                hi = acc[(2 * k + 1) * shard : (2 * k + 2) * shard]
                gmine[b, k, :, cols] = jnp.where(core == 0, lo, hi)
                psend[b, k, :, cols] = jnp.where(core == 0, hi, lo).astype(bf16)
            return carry

        lax.fori_loop(0, width // tile, body, 0)
        return send(psend.at[b], precv.at[b], pair)

    def chip_sum(b, k):
        return gmine[b, k] + precv[b, k].astype(f32)

    pair_d = grad_block(0)
    pair_x = grad_block(1)
    pair_d.wait_recv()
    for k in range(zs):
        dsend[k] = chip_sum(0, k).astype(bf16)
    diag_x = send(dsend.at[pl.ds(0, zh)], rx_diag, xn)
    diag_y = send(dsend.at[pl.ds(zh, zs - zh)], ry_diag, yn)
    pair_y = grad_block(2)
    pair_x.wait_recv()
    for k in range(zh):
        xsend[k] = chip_sum(1, k).astype(bf16)
    x_first = send(xsend.at[pl.ds(0, zh)], rx_block.at[pl.ds(0, zh)], xn)
    pair_y.wait_recv()
    for k in range(zh, zs):
        ysend[k] = chip_sum(2, k).astype(bf16)
    y_second = send(ysend.at[pl.ds(zh, zs - zh)], ry_block.at[pl.ds(zh, zs - zh)], yn)
    pair_o = grad_block(3)
    diag_x.wait_recv()
    for k in range(zh):
        ysend[k] = (chip_sum(2, k) + rx_diag[k].astype(f32)).astype(bf16)
    y_first = send(ysend.at[pl.ds(0, zh)], ry_block.at[pl.ds(0, zh)], yn)
    diag_y.wait_recv()
    for k in range(zh, zs):
        xsend[k] = (chip_sum(1, k) + ry_diag[k - zh].astype(f32)).astype(bf16)
    x_second = send(xsend.at[pl.ds(zh, zs - zh)], rx_block.at[pl.ds(zh, zs - zh)], xn)

    for copy in early:
        copy.wait_recv()
    first_frame = FRAMES_GROUP * group_index[0]
    live_row[...] = jnp.ones_like(live_row)
    for at, held in ((0, frames), (keys_one, frames_recv)):
        f = held[...]
        ok = (f < first_frame) & (f >= first_frame - WINDOW_FRAMES)
        live_row[:, at : at + cached] = jnp.where(ok, 1.0, 0.0)
    live = live_row[...] > 0.5
    rows_q = 2 * zs * own_q
    lane = lax.broadcasted_iota(jnp.int32, (rows_q, 128), 1)
    stats = jnp.zeros((rows_q, 128), f32)
    for h in range(heads_here):
        cols = slice(h * HEAD, (h + 1) * HEAD)
        q_head = q_all[:, :, cols].reshape(rows_q, HEAD)
        scores = lax.dot_general(
            q_head, kfull[:, cols], (((1,), (1,)), ((), ())), preferred_element_type=f32
        ) * (HEAD ** (-0.5))
        scores = jnp.where(live, scores, -1e30)
        top = jnp.max(scores, axis=1, keepdims=True)
        weights = jnp.where(live, jnp.exp(scores - top), 0.0)
        total = jnp.sum(weights, axis=1, keepdims=True)
        summed = jnp.dot(weights.astype(bf16), vfull[:, cols], preferred_element_type=f32)
        asend[:, :, cols] = summed.astype(bf16).reshape(2 * zs, own_q, HEAD)
        stats = jnp.where(lane == h, top, stats)
        stats = jnp.where(lane == 64 + h, total, stats)
    ssend[...] = stats.reshape(2 * zs, own_q, 128)
    late = []
    for j, cc, zt, ct in group:
        peer = (dp, zt * 2 + ct)
        late.append(send(asend.at[zt * 2 + ct], arecv.at[j * 2 + cc], peer))
        late.append(send(ssend.at[zt * 2 + ct], srecv.at[j * 2 + cc], peer))
    arecv[0] = asend[seq]
    srecv[0] = ssend[seq]

    for copy in w_z:
        copy.wait_recv()
    mine = wfull.at[dp, :, core]
    w_x = send(mine, mine, xn)
    w_y = send(mine, mine, yn)
    w_p = send(mine, mine, pair)

    stores = []

    def grad_in_block(b):
        rows = wfull[order[b]].reshape(block, width)
        step = 256

        def body(t, carry):
            at = pl.ds(pl.multiple_of(t * step, step), step)
            gin[b, at] = lax.dot_general(
                cot[at], rows, (((1,), (1,)), ((), ())), preferred_element_type=f32
            ).astype(bf16)
            return carry

        lax.fori_loop(0, tokens // step, body, 0)
        store = pltpu.make_async_copy(
            gin.at[b],
            grad_in_hbm.at[:, pl.ds(pl.multiple_of(order[b] * block, 128), block)],
            local_sems.at[3 + b],
        )
        store.start()
        stores.append(store)

    w_p.wait_recv()
    grad_in_block(3)

    pair_o.wait_recv()
    x_first.wait_recv()
    x_second.wait_recv()
    y_first.wait_recv()
    y_second.wait_recv()
    for k in range(zs):
        osum[k] = chip_sum(3, k) + rx_block[k].astype(f32) + ry_block[k].astype(f32)
    z_parts = []
    for j in range(1, zs):
        zt = lax.rem(z + j, zs)
        zsend[j - 1] = osum[zt].astype(bf16)
        z_parts.append(send(zsend.at[j - 1], zrecv.at[j - 1], (dp, zt * 2 + core)))

    w_x.wait_recv()
    from_x = wfull.at[dp_x, :, core]
    fx = wfull.at[dp_x, pl.ds(0, zh), core]
    w_fy = send(fx, fx, yn)
    w_px = send(from_x, from_x, pair)
    w_y.wait_recv()
    from_y = wfull.at[dp_y, :, core]
    fy = wfull.at[dp_y, pl.ds(zh, zs - zh), core]
    w_fx = send(fy, fy, xn)
    w_py = send(from_y, from_y, pair)

    for copy in late:
        copy.wait_recv()
    for cc in range(2):
        ct = core if cc == 0 else other
        for h in range(heads_here):
            cols = slice(h * HEAD, (h + 1) * HEAD)
            tops = [srecv[j * 2 + cc][:, h : h + 1] for j in range(zs)]
            sums = [srecv[j * 2 + cc][:, 64 + h : 65 + h] for j in range(zs)]
            top = functools.reduce(jnp.maximum, tops)
            acc = jnp.zeros((own_q, HEAD), f32)
            total = jnp.zeros((own_q, 1), f32)
            for j in range(zs):
                scale = jnp.exp(tops[j] - top)
                acc = acc + scale * arecv[j * 2 + cc][:, cols].astype(f32)
                total = total + scale * sums[j]
            at = pl.ds(pl.multiple_of(ct * half + h * HEAD, 128), HEAD)
            mixed[:, at] = (acc / total).astype(bf16)
    loads[2].wait()
    gate = jnp.zeros((1, width), f32)
    for s in range(gate_table.shape[0]):
        gate = gate + jnp.where(timestep[0] == s, gate_table[s : s + 1], 0.0)
    projected = jnp.dot(mixed[...], out_weight[...], preferred_element_type=f32)
    stream_out[...] = (stream[...].astype(f32) + gate * projected).astype(bf16)

    w_px.wait_recv()
    grad_in_block(1)
    w_py.wait_recv()
    grad_in_block(2)

    factor = float(tokens * parts) ** (-0.5)
    for copy in z_parts:
        copy.wait_recv()
    grad = osum[z]
    for j in range(1, zs):
        grad = grad + zrecv[j - 1].astype(f32)
    grad_weight[...] = grad * factor

    w_fy.wait_recv()
    w_fx.wait_recv()
    from_d = wfull.at[dp_d, :, core]
    w_pd = send(from_d, from_d, pair)
    w_pd.wait_recv()
    grad_in_block(0)

    for copy in sent:
        copy.wait_send()
    for store in stores:
        store.wait()


def fused(
    stream,
    queries,
    new_keys,
    new_values,
    cache_keys,
    cache_values,
    cache_frames,
    group_index,
    timestep,
    gate_table,
    attn_out_weight,
    critic_in,
    critic_cot,
    critic_weight,
):
    bf16, f32 = jnp.bfloat16, jnp.float32
    zs = lax.axis_size("seq") // 2
    parts = lax.axis_size(("dp", "seq"))
    tokens, width = critic_in.shape
    own_q = queries.shape[1]
    shard = critic_weight.shape[0]
    cached, fresh = cache_keys.shape[1], new_keys.shape[1]
    half = width // 2
    keys_two = 2 * (cached + fresh)
    zh = zs // 2
    messages = 2 * zs + 4 + (zs - 1) + 4 + 2 + 4 + 2 * (2 * zs - 1) + 3 + (zs - 1) + 4 + 1
    vm = pl.BlockSpec(memory_space=pltpu.VMEM)
    sm = pl.BlockSpec(memory_space=pltpu.SMEM)
    hbm = pl.BlockSpec(memory_space=pl.ANY)
    stream_out, grad_in, grad_weight = pl.pallas_call(
        functools.partial(step_kernel, zs, parts),
        out_shape=(
            jax.ShapeDtypeStruct(stream.shape[1:], bf16),
            jax.ShapeDtypeStruct((tokens, width), bf16),
            jax.ShapeDtypeStruct((shard, width), f32),
        ),
        in_specs=[vm] * 7 + [sm] * 2 + [vm] + [hbm] * 3 + [vm],
        out_specs=(vm, hbm, vm),
        scratch_shapes=[
            pltpu.VMEM((tokens, width), bf16),
            pltpu.VMEM((tokens, width), bf16),
            pltpu.VMEM((width, width), bf16),
            pltpu.VMEM((4, zs, 2, shard, width), bf16),
            pltpu.VMEM((4, zs, shard, width), f32),
            pltpu.VMEM((4, zs, shard, width), bf16),
            pltpu.VMEM((4, zs, shard, width), bf16),
            pltpu.VMEM((zs, shard, width), bf16),
            pltpu.VMEM((zs, shard, width), bf16),
            pltpu.VMEM((zs, shard, width), bf16),
            pltpu.VMEM((zh, shard, width), bf16),
            pltpu.VMEM((zs - zh, shard, width), bf16),
            pltpu.VMEM((zs, shard, width), bf16),
            pltpu.VMEM((zs, shard, width), bf16),
            pltpu.VMEM((zs, shard, width), f32),
            pltpu.VMEM((zs - 1, shard, width), bf16),
            pltpu.VMEM((zs - 1, shard, width), bf16),
            pltpu.VMEM((4, tokens, width // 4), bf16),
            pltpu.VMEM((2 * zs, own_q, half), bf16),
            pltpu.VMEM((keys_two, half), bf16),
            pltpu.VMEM((keys_two, half), bf16),
            pltpu.VMEM((1, cached), jnp.int32),
            pltpu.VMEM((1, keys_two), f32),
            pltpu.VMEM((2 * zs, own_q, half), bf16),
            pltpu.VMEM((2 * zs, own_q, half), bf16),
            pltpu.VMEM((2 * zs, own_q, 128), f32),
            pltpu.VMEM((2 * zs, own_q, 128), f32),
            pltpu.VMEM((own_q, width), bf16),
            pltpu.SemaphoreType.DMA((messages,)),
            pltpu.SemaphoreType.DMA((messages,)),
            pltpu.SemaphoreType.DMA((7,)),
        ],
        compiler_params=pltpu.CompilerParams(
            collective_id=0, has_side_effects=True, vmem_limit_bytes=60 * 1024 * 1024
        ),
    )(
        stream[0],
        queries[0],
        new_keys[0],
        new_values[0],
        cache_keys[0],
        cache_values[0],
        cache_frames,
        group_index,
        timestep,
        gate_table,
        attn_out_weight,
        critic_in,
        critic_cot,
        critic_weight,
    )
    return (stream_out[None], grad_in, grad_weight)


def local(*args):
    shard, tokens = args[13].shape[0], args[11].shape[0]
    fits = (
        lax.axis_size("dp") == 4
        and lax.axis_size("seq") % 4 == 0
        and shard % 16 == 0
        and args[1].shape[1] % 16 == 0
        and args[4].shape[1] % 16 == 0
        and args[1].shape[2] % 512 == 0
        and tokens % 256 == 0
    )
    return fused(*args) if fits else by_collectives(*args)


def solution(mesh):
    return jax.shard_map(
        local,
        mesh=mesh,
        in_specs=(
            P("dp", "seq", None),
            P("dp", "seq", None),
            P("dp", "seq", None),
            P("dp", "seq", None),
            P("dp", "seq", None),
            P("dp", "seq", None),
            P("dp", "seq"),
            P("dp"),
            P("dp"),
            P(),
            P(),
            P(("dp", "seq"), None),
            P(("dp", "seq"), None),
            P(("dp", "seq"), None),
        ),
        out_specs=(P("dp", "seq", None), P(("dp", "seq"), None), P(("dp", "seq"), None)),
        check_vma=False,
    )
```

```python
import functools

import jax
import jax.numpy as jnp
from jax import lax
from jax.experimental import pallas as pl
from jax.experimental.pallas import tpu as pltpu
from jax.sharding import PartitionSpec as P

HEADS = 12
HEAD = 128
FRAMES_GROUP = 3
WINDOW_FRAMES = 9


def critic_pass(critic_in, critic_cot, critic_weight):
    grad_in = lax.dot_general(
        critic_cot,
        lax.all_gather(critic_weight, ("dp", "seq"), axis=0, tiled=True),
        (((1,), (1,)), ((), ())),
        preferred_element_type=jnp.float32,
    ).astype(jnp.bfloat16)
    factor = float(critic_in.shape[0] * lax.axis_size(("dp", "seq"))) ** (-0.5)
    whole_term = (
        lax.dot_general(
            critic_in, critic_cot, (((0,), (0,)), ((), ())), preferred_element_type=jnp.float32
        )
        * factor
    )
    grad_weight = lax.psum_scatter(whole_term, ("dp", "seq"), scatter_dimension=0, tiled=True)
    return (grad_in, grad_weight)


def by_collectives(
    stream,
    queries,
    new_keys,
    new_values,
    cache_keys,
    cache_values,
    cache_frames,
    group_index,
    timestep,
    gate_table,
    attn_out_weight,
    critic_in,
    critic_cot,
    critic_weight,
):
    query_local = queries[0]
    own_rows = query_local.shape[0]
    width = query_local.shape[1]
    scale = HEAD ** (-0.5)
    first_frame = FRAMES_GROUP * group_index[0]
    frames = cache_frames[0]
    live_cache = (frames < first_frame) & (frames >= first_frame - WINDOW_FRAMES)
    live_local = jnp.concatenate([live_cache, jnp.ones((own_rows,), dtype=bool)])
    keys_local = jnp.concatenate([cache_keys[0], new_keys[0]], axis=0)
    values_local = jnp.concatenate([cache_values[0], new_values[0]], axis=0)
    all_queries = lax.all_gather(queries, "seq", axis=1, tiled=True)[0]
    total_rows = all_queries.shape[0]
    query_heads = all_queries.reshape(total_rows, HEADS, HEAD)
    key_heads = keys_local.reshape(-1, HEADS, HEAD)
    value_heads = values_local.reshape(-1, HEADS, HEAD)
    scores = (
        jnp.einsum("qhd,khd->hqk", query_heads, key_heads, preferred_element_type=jnp.float32)
        * scale
    )
    scores = jnp.where(live_local[None, None, :], scores, -1e30)
    local_top = jnp.max(scores, axis=2)
    global_top = lax.pmax(local_top, "seq")
    weights = jnp.where(live_local[None, None, :], jnp.exp(scores - global_top[:, :, None]), 0.0)
    totals = jnp.sum(weights, axis=2)
    summed = jnp.einsum(
        "hqk,khd->qhd",
        weights.astype(jnp.bfloat16),
        value_heads,
        preferred_element_type=jnp.float32,
    )
    own_sums, own_totals = (
        lax.psum_scatter(summed.reshape(total_rows, width), "seq", scatter_dimension=0, tiled=True),
        lax.psum_scatter(totals.T, "seq", scatter_dimension=0, tiled=True),
    )
    mixed = (
        (own_sums.reshape(own_rows, HEADS, HEAD) / own_totals[:, :, None])
        .reshape(own_rows, width)
        .astype(jnp.bfloat16)
    )
    projected = jnp.dot(mixed, attn_out_weight, preferred_element_type=jnp.float32)
    onehot = (
        timestep[:, None] == jnp.arange(gate_table.shape[0], dtype=jnp.int32)[None, :]
    ).astype(jnp.float32)
    gate = jnp.dot(onehot, gate_table, precision=lax.Precision.HIGHEST)
    stream_out = (stream[0].astype(jnp.float32) + gate * projected).astype(jnp.bfloat16)[None]
    grad_in, grad_weight = critic_pass(critic_in, critic_cot, critic_weight)
    return (stream_out, grad_in, grad_weight)


def step_kernel(
    zs,
    parts,
    stream,
    queries,
    new_keys,
    new_values,
    cache_keys,
    cache_values,
    frames,
    group_index,
    timestep,
    gate_table,
    out_weight_hbm,
    critic_in_hbm,
    critic_cot_hbm,
    weight_shard,
    stream_out,
    grad_in_hbm,
    grad_weight,
    diag_rows,
    cin,
    cot,
    out_weight,
    wfull,
    gmine,
    psend,
    precv,
    dsend,
    xsend,
    ysend,
    rx_diag,
    ry_diag,
    rx_block,
    ry_block,
    osum,
    zsend,
    zrecv,
    gin,
    q_all,
    kfull,
    vfull,
    frames_recv,
    live_row,
    asend,
    arecv,
    ssend,
    srecv,
    mixed,
    send_sems,
    recv_sems,
    local_sems,
):
    f32, bf16 = jnp.float32, jnp.bfloat16
    dp, seq = lax.axis_index("dp"), lax.axis_index("seq")
    z, core = seq // 2, lax.rem(seq, 2)
    other = 1 - core
    tokens, width = cin.shape
    block = width // 4
    shard = block // (2 * zs)
    half = width // 2
    own_q = queries.shape[0]
    cached, fresh = cache_keys.shape[0], new_keys.shape[0]
    keys_one = cached + fresh
    heads_here = half // HEAD
    zh = zs // 2
    dp_x = dp + 1 - 2 * lax.rem(dp, 2)
    dp_y = lax.rem(dp + 2, 4)
    dp_d = dp_x + 2 - 4 * (dp_x // 2)
    order = (dp_d, dp_x, dp_y, dp)
    xn, yn, pair = (dp_x, seq), (dp_y, seq), (dp, z * 2 + other)

    loads = [
        pltpu.make_async_copy(critic_in_hbm, cin, local_sems.at[0]),
        pltpu.make_async_copy(critic_cot_hbm, cot, local_sems.at[1]),
        pltpu.make_async_copy(out_weight_hbm, out_weight, local_sems.at[2]),
    ]
    for load in loads:
        load.start()

    group = []
    for j in range(zs):
        for cc in range(2):
            if j or cc:
                zt = lax.rem(z + j, zs)
                ct = core if cc == 0 else other
                group.append((j, cc, zt, ct))
    barrier = pltpu.get_barrier_semaphore()
    peers = [xn, yn] + [(dp, zt * 2 + ct) for (_, _, zt, ct) in group]
    for peer in peers:
        pl.semaphore_signal(
            barrier, inc=1, device_id=peer, device_id_type=pl.DeviceIdType.MESH
        )
    pl.semaphore_wait(barrier, len(peers))

    sent = []

    def send(src, dst, peer):
        n = len(sent)
        copy = pltpu.make_async_remote_copy(
            src_ref=src,
            dst_ref=dst,
            send_sem=send_sems.at[n],
            recv_sem=recv_sems.at[n],
            device_id=peer,
            device_id_type=pl.DeviceIdType.MESH,
        )
        copy.start()
        sent.append(copy)
        return copy

    other_cols = pl.ds(pl.multiple_of(other * half, 128), half)
    own_cols = pl.ds(pl.multiple_of(core * half, 128), half)

    early = []
    for j, cc, zt, ct in group:
        cols = own_cols if cc == 0 else other_cols
        early.append(send(queries.at[:, cols], q_all.at[seq], (dp, zt * 2 + ct)))
    w_z, w_x, w_y, w_p = [], [], [], []
    for j in range(1, zs):
        zt = lax.rem(z + j, zs)
        w_z.append(send(weight_shard, wfull.at[dp, z, core], (dp, zt * 2 + core)))
    for into, peer in ((w_x, xn), (w_y, yn), (w_p, pair)):
        into.append(send(weight_shard, wfull.at[dp, z, core], peer))
    early.append(
        send(cache_keys.at[:, other_cols], kfull.at[pl.ds(keys_one, cached)], pair)
    )
    early.append(
        send(new_keys.at[:, other_cols], kfull.at[pl.ds(keys_one + cached, fresh)], pair)
    )
    early.append(
        send(cache_values.at[:, other_cols], vfull.at[pl.ds(keys_one, cached)], pair)
    )
    early.append(
        send(new_values.at[:, other_cols], vfull.at[pl.ds(keys_one + cached, fresh)], pair)
    )
    early.append(send(frames, frames_recv, pair))

    wfull[dp, z, core] = weight_shard[...]
    q_all[seq] = queries[:, own_cols]
    kfull[0:cached] = cache_keys[:, own_cols]
    kfull[cached:keys_one] = new_keys[:, own_cols]
    vfull[0:cached] = cache_values[:, own_cols]
    vfull[cached:keys_one] = new_values[:, own_cols]

    loads[0].wait()
    loads[1].wait()
    tile = 512 if width % 512 == 0 else 128

    def grad_block(b):
        rows = pl.ds(pl.multiple_of(order[b] * block, 128), block)

        def body(t, carry):
            cols = pl.ds(pl.multiple_of(t * tile, tile), tile)
            acc = lax.dot_general(
                cin[:, rows],
                cot[:, cols],
                (((0,), (0,)), ((), ())),
                preferred_element_type=f32,
            )
            for k in range(zs):
                lo = acc[2 * k * shard : (2 * k + 1) * shard]
                hi = acc[(2 * k + 1) * shard : (2 * k + 2) * shard]
                gmine[b, k, :, cols] = jnp.where(core == 0, lo, hi)
                psend[b, k, :, cols] = jnp.where(core == 0, hi, lo).astype(bf16)
            return carry

        lax.fori_loop(0, width // tile, body, 0)
        return send(psend.at[b], precv.at[b], pair)

    def chip_sum(b, k):
        return gmine[b, k] + precv[b, k].astype(f32)

    pair_d = grad_block(0)
    pair_x = grad_block(1)
    pair_d.wait_recv()
    for k in range(zs):
        dsend[k] = chip_sum(0, k).astype(bf16)
    diag_x = send(dsend.at[pl.ds(0, zh)], rx_diag, xn)
    diag_y = send(dsend.at[pl.ds(zh, zs - zh)], ry_diag, yn)
    pair_y = grad_block(2)
    pair_x.wait_recv()
    for k in range(zh):
        xsend[k] = chip_sum(1, k).astype(bf16)
    x_first = send(xsend.at[pl.ds(0, zh)], rx_block.at[pl.ds(0, zh)], xn)
    pair_y.wait_recv()
    for k in range(zh, zs):
        ysend[k] = chip_sum(2, k).astype(bf16)
    y_second = send(ysend.at[pl.ds(zh, zs - zh)], ry_block.at[pl.ds(zh, zs - zh)], yn)
    pair_o = grad_block(3)
    diag_x.wait_recv()
    for k in range(zh):
        ysend[k] = (chip_sum(2, k) + rx_diag[k].astype(f32)).astype(bf16)
    y_first = send(ysend.at[pl.ds(0, zh)], ry_block.at[pl.ds(0, zh)], yn)
    diag_y.wait_recv()
    for k in range(zh, zs):
        xsend[k] = (chip_sum(1, k) + ry_diag[k - zh].astype(f32)).astype(bf16)
    x_second = send(xsend.at[pl.ds(zh, zs - zh)], rx_block.at[pl.ds(zh, zs - zh)], xn)

    for j in range(1, zs):
        w_z[j - 1].wait_recv()
        held = wfull.at[dp, lax.rem(z + zs - j, zs), core]
        for into, peer in ((w_x, xn), (w_y, yn), (w_p, pair)):
            into.append(send(held, held, peer))

    for copy in early:
        copy.wait_recv()
    first_frame = FRAMES_GROUP * group_index[0]
    live_row[...] = jnp.ones_like(live_row)
    for at, held in ((0, frames), (keys_one, frames_recv)):
        f = held[...]
        ok = (f < first_frame) & (f >= first_frame - WINDOW_FRAMES)
        live_row[:, at : at + cached] = jnp.where(ok, 1.0, 0.0)
    live = live_row[...] > 0.5
    rows_q = 2 * zs * own_q
    lane = lax.broadcasted_iota(jnp.int32, (rows_q, 128), 1)
    stats = jnp.zeros((rows_q, 128), f32)
    for h in range(heads_here):
        cols = slice(h * HEAD, (h + 1) * HEAD)
        q_head = q_all[:, :, cols].reshape(rows_q, HEAD)
        scores = lax.dot_general(
            q_head, kfull[:, cols], (((1,), (1,)), ((), ())), preferred_element_type=f32
        ) * (HEAD ** (-0.5))
        scores = jnp.where(live, scores, -1e30)
        top = jnp.max(scores, axis=1, keepdims=True)
        weights = jnp.where(live, jnp.exp(scores - top), 0.0)
        total = jnp.sum(weights, axis=1, keepdims=True)
        summed = jnp.dot(weights.astype(bf16), vfull[:, cols], preferred_element_type=f32)
        asend[:, :, cols] = summed.astype(bf16).reshape(2 * zs, own_q, HEAD)
        stats = jnp.where(lane == h, top, stats)
        stats = jnp.where(lane == 64 + h, total, stats)
    ssend[...] = stats.reshape(2 * zs, own_q, 128)
    late = []
    for j, cc, zt, ct in group:
        peer = (dp, zt * 2 + ct)
        late.append(send(asend.at[zt * 2 + ct], arecv.at[j * 2 + cc], peer))
        late.append(send(ssend.at[zt * 2 + ct], srecv.at[j * 2 + cc], peer))
    arecv[0] = asend[seq]
    srecv[0] = ssend[seq]

    w_px, w_py, w_diag = [], [], []

    def pass_on(j):
        zf = lax.rem(z + zs - j, zs)
        w_x[j].wait_recv()
        held = wfull.at[dp_x, zf, core]
        if j < zh:
            w_diag.append(send(held, held, yn))
        w_px.append(send(held, held, pair))
        w_y[j].wait_recv()
        held = wfull.at[dp_y, zf, core]
        if j >= zh:
            w_diag.append(send(held, held, xn))
        w_py.append(send(held, held, pair))

    stores = []

    def grad_in_block(b):
        rows = wfull[order[b]].reshape(block, width)
        step = 256

        def body(t, carry):
            at = pl.ds(pl.multiple_of(t * step, step), step)
            gin[b, at] = lax.dot_general(
                cot[at], rows, (((1,), (1,)), ((), ())), preferred_element_type=f32
            ).astype(bf16)
            return carry

        lax.fori_loop(0, tokens // step, body, 0)
        store = pltpu.make_async_copy(
            gin.at[b],
            grad_in_hbm.at[:, pl.ds(pl.multiple_of(order[b] * block, 128), block)],
            local_sems.at[3 + b],
        )
        store.start()
        stores.append(store)

    pass_on(0)
    for copy in w_p:
        copy.wait_recv()
    grad_in_block(3)

    pair_o.wait_recv()
    x_first.wait_recv()
    x_second.wait_recv()
    y_first.wait_recv()
    y_second.wait_recv()
    for k in range(zs):
        osum[k] = chip_sum(3, k) + rx_block[k].astype(f32) + ry_block[k].astype(f32)
    z_parts = []
    for j in range(1, zs):
        zt = lax.rem(z + j, zs)
        zsend[j - 1] = osum[zt].astype(bf16)
        z_parts.append(send(zsend.at[j - 1], zrecv.at[j - 1], (dp, zt * 2 + core)))

    for j in range(1, zs):
        pass_on(j)

    for copy in late:
        copy.wait_recv()
    for cc in range(2):
        ct = core if cc == 0 else other
        for h in range(heads_here):
            cols = slice(h * HEAD, (h + 1) * HEAD)
            tops = [srecv[j * 2 + cc][:, h : h + 1] for j in range(zs)]
            sums = [srecv[j * 2 + cc][:, 64 + h : 65 + h] for j in range(zs)]
            top = functools.reduce(jnp.maximum, tops)
            acc = jnp.zeros((own_q, HEAD), f32)
            total = jnp.zeros((own_q, 1), f32)
            for j in range(zs):
                scale = jnp.exp(tops[j] - top)
                acc = acc + scale * arecv[j * 2 + cc][:, cols].astype(f32)
                total = total + scale * sums[j]
            at = pl.ds(pl.multiple_of(ct * half + h * HEAD, 128), HEAD)
            mixed[:, at] = (acc / total).astype(bf16)
    loads[2].wait()
    gate = jnp.zeros((1, width), f32)
    for s in range(gate_table.shape[0]):
        gate = gate + jnp.where(timestep[0] == s, gate_table[s : s + 1], 0.0)
    projected = jnp.dot(mixed[...], out_weight[...], preferred_element_type=f32)
    stream_out[...] = (stream[...].astype(f32) + gate * projected).astype(bf16)

    for copy in w_px:
        copy.wait_recv()
    grad_in_block(1)
    for copy in w_py:
        copy.wait_recv()
    grad_in_block(2)
    w_pd = []
    for j in range(zs):
        w_diag[j].wait_recv()
        held = wfull.at[dp_d, lax.rem(z + zs - j, zs), core]
        w_pd.append(send(held, held, pair))

    factor = float(tokens * parts) ** (-0.5)
    for copy in z_parts:
        copy.wait_recv()
    grad = osum[z]
    for j in range(1, zs):
        grad = grad + zrecv[j - 1].astype(f32)
    grad_weight[...] = grad * factor

    for copy in w_pd:
        copy.wait_recv()
    keep = pltpu.make_async_copy(wfull.at[dp_d], diag_rows, local_sems.at[3])
    keep.start()
    stores.append(keep)

    for copy in sent:
        copy.wait_send()
    for store in stores:
        store.wait()


def finish_kernel(stream_part, weight_part, grad_part, cot, diag_rows, stream_out, grad_weight, grad_in):
    stream_out[...] = stream_part[...]
    grad_weight[...] = weight_part[...]
    grad_in[...] = grad_part[...]
    width = cot.shape[1]
    block = width // 4
    dp = lax.axis_index("dp")
    dp_x = dp + 1 - 2 * lax.rem(dp, 2)
    dp_d = dp_x + 2 - 4 * (dp_x // 2)
    rows = diag_rows[...].reshape(block, width)
    grad_in[:, pl.ds(pl.multiple_of(dp_d * block, 128), block)] = lax.dot_general(
        cot[...], rows, (((1,), (1,)), ((), ())), preferred_element_type=jnp.float32
    ).astype(grad_in.dtype)


def fused(
    stream,
    queries,
    new_keys,
    new_values,
    cache_keys,
    cache_values,
    cache_frames,
    group_index,
    timestep,
    gate_table,
    attn_out_weight,
    critic_in,
    critic_cot,
    critic_weight,
):
    bf16, f32 = jnp.bfloat16, jnp.float32
    zs = lax.axis_size("seq") // 2
    parts = lax.axis_size(("dp", "seq"))
    tokens, width = critic_in.shape
    own_q = queries.shape[1]
    shard = critic_weight.shape[0]
    cached, fresh = cache_keys.shape[1], new_keys.shape[1]
    half = width // 2
    keys_two = 2 * (cached + fresh)
    zh = zs // 2
    messages = (2 * zs - 1) * 3 + 5 + (zs - 1) * 2 + 10 + 7 * zs
    vm = pl.BlockSpec(memory_space=pltpu.VMEM)
    sm = pl.BlockSpec(memory_space=pltpu.SMEM)
    hbm = pl.BlockSpec(memory_space=pl.ANY)
    stream_part, grad_part, weight_part, diag_rows = pl.pallas_call(
        functools.partial(step_kernel, zs, parts),
        out_shape=(
            jax.ShapeDtypeStruct(stream.shape[1:], bf16),
            jax.ShapeDtypeStruct((tokens, width), bf16),
            jax.ShapeDtypeStruct((shard, width), f32),
            jax.ShapeDtypeStruct((zs, 2, shard, width), bf16),
        ),
        in_specs=[vm] * 7 + [sm] * 2 + [vm] + [hbm] * 3 + [vm],
        out_specs=(vm, hbm, vm, hbm),
        scratch_shapes=[
            pltpu.VMEM((tokens, width), bf16),
            pltpu.VMEM((tokens, width), bf16),
            pltpu.VMEM((width, width), bf16),
            pltpu.VMEM((4, zs, 2, shard, width), bf16),
            pltpu.VMEM((4, zs, shard, width), f32),
            pltpu.VMEM((4, zs, shard, width), bf16),
            pltpu.VMEM((4, zs, shard, width), bf16),
            pltpu.VMEM((zs, shard, width), bf16),
            pltpu.VMEM((zs, shard, width), bf16),
            pltpu.VMEM((zs, shard, width), bf16),
            pltpu.VMEM((zh, shard, width), bf16),
            pltpu.VMEM((zs - zh, shard, width), bf16),
            pltpu.VMEM((zs, shard, width), bf16),
            pltpu.VMEM((zs, shard, width), bf16),
            pltpu.VMEM((zs, shard, width), f32),
            pltpu.VMEM((zs - 1, shard, width), bf16),
            pltpu.VMEM((zs - 1, shard, width), bf16),
            pltpu.VMEM((4, tokens, width // 4), bf16),
            pltpu.VMEM((2 * zs, own_q, half), bf16),
            pltpu.VMEM((keys_two, half), bf16),
            pltpu.VMEM((keys_two, half), bf16),
            pltpu.VMEM((1, cached), jnp.int32),
            pltpu.VMEM((1, keys_two), f32),
            pltpu.VMEM((2 * zs, own_q, half), bf16),
            pltpu.VMEM((2 * zs, own_q, half), bf16),
            pltpu.VMEM((2 * zs, own_q, 128), f32),
            pltpu.VMEM((2 * zs, own_q, 128), f32),
            pltpu.VMEM((own_q, width), bf16),
            pltpu.SemaphoreType.DMA((messages,)),
            pltpu.SemaphoreType.DMA((messages,)),
            pltpu.SemaphoreType.DMA((7,)),
        ],
        compiler_params=pltpu.CompilerParams(
            collective_id=0, has_side_effects=True, vmem_limit_bytes=60 * 1024 * 1024
        ),
    )(
        stream[0],
        queries[0],
        new_keys[0],
        new_values[0],
        cache_keys[0],
        cache_values[0],
        cache_frames,
        group_index,
        timestep,
        gate_table,
        attn_out_weight,
        critic_in,
        critic_cot,
        critic_weight,
    )
    rows = 256

    def whole(shape):
        return pl.BlockSpec(shape, lambda i: (0,) * len(shape))

    tiles = pl.BlockSpec((rows, width), lambda i: (i, 0))
    small = [whole((own_q, width)), whole((shard, width))]
    stream_out, grad_weight, grad_in = pl.pallas_call(
        finish_kernel,
        grid=(tokens // rows,),
        out_shape=(
            jax.ShapeDtypeStruct((own_q, width), bf16),
            jax.ShapeDtypeStruct((shard, width), f32),
            jax.ShapeDtypeStruct((tokens, width), bf16),
        ),
        in_specs=small + [tiles, tiles, whole((zs, 2, shard, width))],
        out_specs=tuple(small + [tiles]),
    )(stream_part, weight_part, grad_part, critic_cot, diag_rows)
    return (stream_out[None], grad_in, grad_weight)


def local(*args):
    shard, tokens = args[13].shape[0], args[11].shape[0]
    fits = (
        lax.axis_size("dp") == 4
        and lax.axis_size("seq") % 4 == 0
        and shard % 16 == 0
        and args[1].shape[1] % 16 == 0
        and args[4].shape[1] % 16 == 0
        and args[1].shape[2] % 512 == 0
        and tokens % 256 == 0
    )
    return fused(*args) if fits else by_collectives(*args)


def solution(mesh):
    return jax.shard_map(
        local,
        mesh=mesh,
        in_specs=(
            P("dp", "seq", None),
            P("dp", "seq", None),
            P("dp", "seq", None),
            P("dp", "seq", None),
            P("dp", "seq", None),
            P("dp", "seq", None),
            P("dp", "seq"),
            P("dp"),
            P("dp"),
            P(),
            P(),
            P(("dp", "seq"), None),
            P(("dp", "seq"), None),
            P(("dp", "seq"), None),
        ),
        out_specs=(P("dp", "seq", None), P(("dp", "seq"), None), P(("dp", "seq"), None)),
        check_vma=False,
    )
```
